32 devices in a mesh: parts: 2 (over y), modes: 16 (over z, x, core).
Axes of the slice: x: 2, y: 2, z: 4, core: 2. Of those that a mesh axis runs over, the one named last changes fastest.
Arguments:
- stem: bfloat16 [2, 16, 64, 32, 512], P(None, 'modes', None, None, 'parts'), parts along dimension 4, may hold values from -6 to 6
- branch_one: bfloat16 [2, 1024, 1024], replicated, may hold values from -0.125 to 0.125
- branch_two: bfloat16 [2, 1024, 1024], replicated, may hold values from -0.125 to 0.125
- branch_three: bfloat16 [2, 2, 16, 512, 512], P(None, None, 'modes'), may hold values from -0.0625 to 0.0625
- leg_orders: int32 [2, 10], replicated, may hold values from 0 to 9, each once within a row
- slice_pick: int32 [32], P('parts'), parts along dimension 0, may hold values from 0 to 1
Outputs:
- contracted: bfloat16 [1024, 2, 2, 2, 256], P(('parts', 'modes')), parts along dimension 0
The draws below stay inside these ranges and needn't reach their ends.
There are 2 independent parts, one for each index of `parts`. The reference program is written for one: setup_inputs(seed, part) draws one part's arguments, and reference() takes and returns one part's arrays. A program takes and returns all parts, laid end to end along the dimension named above; an argument that names none is the same for every part. Nothing has to cross between parts.
Inputs may be any that keep to these rules, and one draw needn't show every extreme that they name: `leg_orders`: each row names every input leg bit once.
All inputs are finite; a program needn't handle non-finite values.
Results may differ from the reference program's by a relative error of at most 0.008.
Values may be sent and summed in bfloat16 or wider, within the bound.
A program may use at most 128 MiB of HBM per device.

```python
import jax
import jax.numpy as jnp

LEGS = 10
C = 1024
OUTW = 512
SLICES = 2
ROWS_DEV = 2
L = 256
E = 64
H = 32
N_MODES = 16


def with_ends(values, own_key, low, top_value):
    shape = values.shape
    place = [jax.random.randint(jax.random.fold_in(own_key, axis), (), 0, shape[axis]) for axis in range(len(shape))]
    values = values.at[tuple(place)].set(low)
    longest = shape.index(max(shape))
    place[longest] = (place[longest] + 1) % shape[longest]
    return values.at[tuple(place)].set(top_value)


def raised(drawn, key, source, target, blocks, factor):
    def block_of(dim):
        return (jnp.arange(drawn.shape[dim]) // (drawn.shape[dim] // blocks)).reshape((-1,) + (1,) * (drawn.ndim - 1 - dim))

    one_side = jax.random.permutation(key, blocks)[block_of(target)]
    other_side = (block_of(target) + blocks // 2) % blocks
    return jnp.where((block_of(source) == one_side) | (block_of(source) == other_side), factor * drawn, drawn)


def levels(stream_key, extent, shards, low, largest):
    def one(axis_at, parts):
        heights = jax.random.uniform(jax.random.fold_in(jax.random.fold_in(stream_key, 6), axis_at), (parts,), jnp.float32, low / len(shards), largest / len(shards))
        return jnp.repeat(jnp.exp(heights), extent[axis_at] // parts).reshape((-1,) + (1,) * (len(extent) - axis_at - 1))

    factor_of = one(*shards[0])
    for cut in shards[1:]:
        factor_of = factor_of * one(*cut)
    return factor_of


def bell_draw(rng, shape, deviation, bound, shards=(), kind=jnp.bfloat16):
    gain = levels(rng, shape, shards, -0.22, 0.18) if shards else 1.0
    drawn = jax.random.normal(rng, shape, jnp.float32) * deviation * gain
    return jnp.minimum(jnp.maximum(drawn, -bound), bound).astype(kind)


def gaussian_with(key, dims, width, most, pieces, heavy, kind=jnp.bfloat16):
    values = width * jax.random.normal(key, dims, jnp.float32)
    if pieces:
        values = values * levels(key, dims, pieces, -0.22, 0.18)
    return jnp.clip(raised(values, jax.random.fold_in(key, 3), *heavy), -most, most).astype(kind)


def setup_inputs(seed: int = 0, part: int = 0) -> dict:
    splits = jax.random.split(jax.random.key(seed), 7)
    own_keys = jax.random.split(jax.random.fold_in(splits[6], part), 7)
    stem = bell_draw(own_keys[0], (2, N_MODES, E, H, L), 1.0, 6.0, ((1, 16),))
    branch_one = bell_draw(splits[1], (2, C, C), (2 * C) ** -0.5, 0.125)
    branch_two = bell_draw(splits[2], (2, C, C), (2 * C) ** -0.5, 0.125)
    branch_three = gaussian_with(splits[3], (SLICES, 2, N_MODES, OUTW, C // 2), (N_MODES * C) ** -0.5, 0.0625, ((2, 16),), (2, 3, 16, 2.0))
    leg_orders = jax.vmap(lambda own: jax.random.permutation(own, LEGS))(jax.random.split(splits[4], 2)).reshape((2, LEGS)).astype(jnp.int32)
    slice_pick = with_ends(jax.random.randint(own_keys[5], (N_MODES,), 0, SLICES), jax.random.fold_in(own_keys[5], 1), 0, SLICES - 1).astype(jnp.int32)
    return dict(stem=stem, branch_one=branch_one, branch_two=branch_two, branch_three=branch_three, leg_orders=leg_orders, slice_pick=slice_pick)


def leg_index(order, leg_width):
    positions = jnp.arange(leg_width, dtype=jnp.int32)
    shifts = jnp.arange(order.shape[0], dtype=jnp.int32)
    digits = jnp.right_shift(positions[:, None], shifts[None, :]) % 2
    placed = jnp.left_shift(digits, order[None, :].astype(jnp.int32))
    return jnp.sum(placed, axis=1).astype(jnp.int32)


def complex_apply(weight, values):
    real_part = weight[0]
    imag_part = weight[1]
    block_matrix = jnp.concatenate([jnp.concatenate([real_part, -imag_part], axis=1), jnp.concatenate([imag_part, real_part], axis=1)], axis=0)
    stacked = values.reshape(2 * values.shape[1], values.shape[2])
    result = jnp.dot(block_matrix, stacked, preferred_element_type=jnp.float32)
    return result.reshape(2, weight.shape[1], values.shape[2])


def reference(stem, branch_one, branch_two, branch_three, leg_orders, slice_pick):
    groups = N_MODES
    half_width = C // 2
    quarter = groups // 4
    columns = ROWS_DEV * groups * L
    values = stem.reshape(2, C, columns)
    weight_one = jnp.take(branch_one, leg_index(leg_orders[0], C), axis=2)
    after_first = complex_apply(weight_one, values).astype(jnp.bfloat16)
    after_first = after_first.reshape(2, 2, half_width, 2, quarter, 2, ROWS_DEV, L)
    second_in = after_first.transpose(0, 3, 2, 1, 4, 5, 6, 7).reshape(2, C, columns)
    weight_two = jnp.take(branch_two, leg_index(leg_orders[1], C), axis=2)
    after_second = complex_apply(weight_two, second_in).astype(jnp.bfloat16)
    after_second = after_second.reshape(2, 2, half_width, 2, quarter, 2, ROWS_DEV, L)
    third_in = after_second.transpose(0, 3, 4, 6, 2, 1, 5, 7).reshape(2, groups * half_width, 4 * L)
    split_ids = jnp.arange(groups, dtype=jnp.int32)
    picked = branch_three[slice_pick.astype(jnp.int32), :, split_ids]
    chosen = picked.transpose(1, 0, 2, 3)
    weight_three = chosen.transpose(0, 2, 1, 3).reshape(2, OUTW, groups * half_width)
    after_third = complex_apply(weight_three, third_in)
    return after_third.reshape(2, OUTW, 2, 2, L).transpose(1, 0, 2, 3, 4).astype(jnp.bfloat16)
```

```python
import jax
import jax.numpy as jnp
from jax import lax
from jax.experimental import pallas as pl
from jax.experimental.pallas import tpu as pltpu
from jax.sharding import PartitionSpec as P

TILES = 4


def leg_index(order, leg_width):
    positions = jnp.arange(leg_width, dtype=jnp.int32)
    shifts = jnp.arange(order.shape[0], dtype=jnp.int32)
    digits = jnp.right_shift(positions[:, None], shifts[None, :]) % 2
    placed = jnp.left_shift(digits, order[None, :])
    return jnp.sum(placed, axis=1)


def turned(branch, order):
    width = branch.shape[2]
    source = leg_index(order, width)
    rows = lax.broadcasted_iota(jnp.int32, (width, width), 0)
    onehot = (rows == source[None, :]).astype(branch.dtype)
    flat = branch.reshape(-1, width)
    out = jnp.dot(flat, onehot, preferred_element_type=jnp.float32)
    return out.astype(branch.dtype).reshape(branch.shape)


def complex_tile(w, values):
    half = values.shape[1] // 2
    p = jnp.dot(w[0], values, preferred_element_type=jnp.float32)
    q = jnp.dot(w[1], values, preferred_element_type=jnp.float32)
    real = p[:, :half] - q[:, half:]
    imag = p[:, half:] + q[:, :half]
    return real.astype(jnp.bfloat16), imag.astype(jnp.bfloat16)


def two_branches(x_hbm, w1_hbm, w2_hbm, out, x, w1, w2, mid, sems):
    width = x.shape[0]
    half = width // 2
    tile = width // TILES
    lanes = x.shape[1] // 8
    copies = [pltpu.make_async_copy(x_hbm, x, sems.at[0])]
    for which, (source, target) in enumerate(((w1_hbm, w1), (w2_hbm, w2))):
        for i in range(TILES):
            rows = pl.ds(i * tile, tile)
            copies.append(
                pltpu.make_async_copy(
                    source.at[:, rows, :], target.at[:, rows, :], sems.at[1 + which * TILES + i]
                )
            )
    for copy in copies:
        copy.start()
    copies[0].wait()
    for i in range(TILES):
        copies[1 + i].wait()
        t, c = divmod(i * tile, half)
        parts = complex_tile(w1[:, i * tile : (i + 1) * tile, :], x[...])
        for r in range(2):
            for a in range(2):
                at = (2 * r + t) * 2 * lanes
                mid[a * half + c : a * half + c + tile, at : at + 2 * lanes] = parts[r][
                    :, a * 2 * lanes : (a + 1) * 2 * lanes
                ]
    for i in range(TILES):
        copies[1 + TILES + i].wait()
        u, c = divmod(i * tile, half)
        parts = complex_tile(w2[:, i * tile : (i + 1) * tile, :], mid[...])
        for r in range(2):
            for td in range(4):
                at = (2 * r + u) * lanes
                out[td, c : c + tile, at : at + lanes] = parts[r][:, td * lanes : (td + 1) * lanes]


def third_branch(place, wa, wb, wc, wd, values, out):
    k2 = place[0]
    k0 = place[1]
    half = values.shape[2] // 2
    p = q = None
    for w, t, d in ((wa, k2, k0), (wb, 1 - k2, k0), (wc, k2, 1 - k0), (wd, 1 - k2, 1 - k0)):
        block = values[2 * t + d]
        pp = jnp.dot(w[0], block, preferred_element_type=jnp.float32)
        qq = jnp.dot(w[1], block, preferred_element_type=jnp.float32)
        p = pp if p is None else p + pp
        q = qq if q is None else q + qq
    out[:, :half] = (p[:, :half] - q[:, half:]).astype(out.dtype)
    out[:, half:] = (p[:, half:] + q[:, :half]).astype(out.dtype)


def per_device(stem, branch_one, branch_two, branch_three, leg_orders, slice_pick):
    groups = lax.axis_size("modes")
    me = lax.axis_index("modes")
    rest = groups // 8
    entries, lanes = stem.shape[2], stem.shape[4] // 2
    k2 = (me // (2 * rest)) % 2
    quarter = me // (2 * rest)
    k0 = me % 2

    cut = stem.reshape(2, entries, 2, 2, rest, 2, 2, 2, lanes)
    cut = cut.transpose(3, 7, 4, 5, 1, 0, 2, 6, 8).reshape(groups, entries, 8 * lanes)
    arrived = lax.all_to_all(cut, "modes", split_axis=0, concat_axis=0, tiled=True)
    x = arrived.reshape(groups * entries, 8 * lanes)

    pick = lax.dynamic_index_in_dim(slice_pick, me, 0, keepdims=False)
    own = lax.dynamic_index_in_dim(branch_three, pick, 0, keepdims=False)[:, 0]
    q = 2 * rest
    middle = [(q + i, 2 * q + i) for i in range(q)]
    middle += [(b, a) for a, b in middle]
    outer = [(i, i ^ q) for i in range(groups)] if q & (q - 1) == 0 else [
        (i, i + q if (i // q) % 2 == 0 else i - q) for i in range(groups)
    ]
    cores = [(i, i ^ 1) for i in range(groups)]
    crossed = lax.ppermute(own, "modes", middle)
    inner = (quarter == 1) | (quarter == 2)
    wa = jnp.where(inner, crossed, own)
    wb = lax.ppermute(wa, "modes", outer)
    wc = lax.ppermute(wa, "modes", cores)
    wd = lax.ppermute(wb, "modes", cores)

    w1 = turned(branch_one, leg_orders[0])
    w2 = turned(branch_two, leg_orders[1])
    width = w1.shape[1]
    half = width // 2
    any_spec = pl.BlockSpec(memory_space=pl.ANY)
    vmem = pl.BlockSpec(memory_space=pltpu.VMEM)
    values = pl.pallas_call(
        two_branches,
        name="two_branches",
        out_shape=jax.ShapeDtypeStruct((4, half, 4 * lanes), jnp.bfloat16),
        in_specs=[any_spec] * 3,
        out_specs=vmem,
        scratch_shapes=[
            pltpu.VMEM(x.shape, x.dtype),
            pltpu.VMEM(w1.shape, w1.dtype),
            pltpu.VMEM(w2.shape, w2.dtype),
            pltpu.VMEM((width, 8 * lanes), jnp.bfloat16),
            pltpu.SemaphoreType.DMA((1 + 2 * TILES,)),
        ],
        compiler_params=pltpu.CompilerParams(vmem_limit_bytes=40 * 2**20),
        cost_estimate=pl.CostEstimate(
            flops=8 * width * width * 8 * lanes, bytes_accessed=12 * 2**20, transcendentals=0
        ),
    )(x, w1, w2)

    out_width = own.shape[1]
    partial = pl.pallas_call(
        third_branch,
        name="third_branch",
        out_shape=jax.ShapeDtypeStruct((out_width, 4 * lanes), jnp.bfloat16),
        in_specs=[pl.BlockSpec(memory_space=pltpu.SMEM)] + [vmem] * 5,
        out_specs=vmem,
        compiler_params=pltpu.CompilerParams(vmem_limit_bytes=24 * 2**20),
        cost_estimate=pl.CostEstimate(
            flops=16 * out_width * half * 4 * lanes, bytes_accessed=7 * 2**20, transcendentals=0
        ),
    )(jnp.stack([k2, k0]).astype(jnp.int32), wa, wb, wc, wd, values)

    pieces = lax.all_to_all(partial, "modes", split_axis=0, concat_axis=0, tiled=True)
    mine = out_width // groups
    pieces = pieces.reshape(2, 2, rest, 2, mine, 2, 2, lanes).astype(jnp.float32)
    summed = jnp.sum(pieces, axis=(0, 2)).astype(jnp.bfloat16)
    return summed.transpose(2, 3, 4, 1, 0, 5).reshape(mine, 2, 2, 2, 2 * lanes)


def solution(mesh):
    in_specs = (
        P(None, "modes", None, None, "parts"),
        P(),
        P(),
        P(None, None, "modes", None, None),
        P(),
        P("parts"),
    )
    out_specs = P(("parts", "modes"), None, None, None, None)
    return jax.shard_map(
        per_device, mesh=mesh, in_specs=in_specs, out_specs=out_specs, check_vma=False
    )
```

```python
import jax
import jax.numpy as jnp
from jax import lax
from jax.experimental import pallas as pl
from jax.experimental.pallas import tpu as pltpu
from jax.sharding import PartitionSpec as P

TILES = 4


def turn_columns(order, branch, out, onehot):
    width = branch.shape[1]

    @pl.when(pl.program_id(0) == 0)
    def _():
        positions = lax.broadcasted_iota(jnp.int32, (1, width), 1)
        source = jnp.zeros((1, width), jnp.int32)
        for bit in range(order.shape[0]):
            source += jnp.left_shift(jnp.right_shift(positions, bit) & 1, order[bit])
        rows = lax.broadcasted_iota(jnp.int32, (width, width), 0)
        onehot[...] = jnp.where(rows == source, 1.0, 0.0).astype(onehot.dtype)

    out[...] = jnp.dot(
        branch[...], onehot[...], preferred_element_type=jnp.float32
    ).astype(out.dtype)


def turned(branch, order, name):
    width = branch.shape[2]
    flat = branch.reshape(-1, width)
    tile = flat.shape[0] // 8
    out = pl.pallas_call(
        turn_columns,
        name=name,
        grid=(8,),
        out_shape=jax.ShapeDtypeStruct(flat.shape, flat.dtype),
        in_specs=[
            pl.BlockSpec(memory_space=pltpu.SMEM),
            pl.BlockSpec((tile, width), lambda i: (i, 0)),
        ],
        out_specs=pl.BlockSpec((tile, width), lambda i: (i, 0)),
        scratch_shapes=[pltpu.VMEM((width, width), flat.dtype)],
        compiler_params=pltpu.CompilerParams(vmem_limit_bytes=58 * 2**20),
        cost_estimate=pl.CostEstimate(
            flops=2 * flat.shape[0] * width * width,
            bytes_accessed=4 * flat.size,
            transcendentals=0,
        ),
    )(order, flat)
    return out.reshape(branch.shape)


def complex_tile(w, values):
    half = values.shape[1] // 2
    p = jnp.dot(w[0], values, preferred_element_type=jnp.float32)
    q = jnp.dot(w[1], values, preferred_element_type=jnp.float32)
    real = p[:, :half] - q[:, half:]
    imag = p[:, half:] + q[:, :half]
    return real.astype(jnp.bfloat16), imag.astype(jnp.bfloat16)


def two_branches(x_hbm, w1_hbm, w2_hbm, out, x, w1, w2, mid, sems):
    width = x.shape[0]
    half = width // 2
    tile = width // TILES
    lanes = x.shape[1] // 8
    copies = [pltpu.make_async_copy(x_hbm, x, sems.at[0])]
    for which, (source, target) in enumerate(((w1_hbm, w1), (w2_hbm, w2))):
        for i in range(TILES):
            rows = pl.ds(i * tile, tile)
            copies.append(
                pltpu.make_async_copy(
                    source.at[:, rows, :], target.at[:, rows, :], sems.at[1 + which * TILES + i]
                )
            )
    for copy in copies:
        copy.start()
    copies[0].wait()
    for i in range(TILES):
        copies[1 + i].wait()
        t, c = divmod(i * tile, half)
        parts = complex_tile(w1[:, i * tile : (i + 1) * tile, :], x[...])
        for r in range(2):
            for a in range(2):
                at = (2 * r + t) * 2 * lanes
                mid[a * half + c : a * half + c + tile, at : at + 2 * lanes] = parts[r][
                    :, a * 2 * lanes : (a + 1) * 2 * lanes
                ]
    for i in range(TILES):
        copies[1 + TILES + i].wait()
        u, c = divmod(i * tile, half)
        parts = complex_tile(w2[:, i * tile : (i + 1) * tile, :], mid[...])
        for r in range(2):
            for td in range(4):
                at = (2 * r + u) * lanes
                out[td, c : c + tile, at : at + lanes] = parts[r][:, td * lanes : (td + 1) * lanes]


def third_branch(place, wa, wb, wc, wd, values, out):
    k2 = place[0]
    k0 = place[1]
    half = values.shape[2] // 2
    p = q = None
    for w, t, d in ((wa, k2, k0), (wb, 1 - k2, k0), (wc, k2, 1 - k0), (wd, 1 - k2, 1 - k0)):
        block = values[2 * t + d]
        pp = jnp.dot(w[0], block, preferred_element_type=jnp.float32)
        qq = jnp.dot(w[1], block, preferred_element_type=jnp.float32)
        p = pp if p is None else p + pp
        q = qq if q is None else q + qq
    out[:, :half] = (p[:, :half] - q[:, half:]).astype(out.dtype)
    out[:, half:] = (p[:, half:] + q[:, :half]).astype(out.dtype)


def per_device(stem, branch_one, branch_two, branch_three, leg_orders, slice_pick):
    groups = lax.axis_size("modes")
    me = lax.axis_index("modes")
    rest = groups // 8
    entries, lanes = stem.shape[2], stem.shape[4] // 2
    k2 = (me // (2 * rest)) % 2
    quarter = me // (2 * rest)
    k0 = me % 2

    cut = stem.reshape(2, entries, 2, 2, rest, 2, 2, 2, lanes)
    cut = cut.transpose(3, 7, 4, 5, 1, 0, 2, 6, 8).reshape(groups, entries, 8 * lanes)
    pick = lax.dynamic_index_in_dim(slice_pick, me, 0, keepdims=False)
    own = lax.dynamic_index_in_dim(branch_three, pick, 0, keepdims=False)[:, 0]
    q = 2 * rest
    middle = [(q + i, 2 * q + i) for i in range(q)]
    middle += [(b, a) for a, b in middle]
    outer = [(i, i ^ q) for i in range(groups)] if q & (q - 1) == 0 else [
        (i, i + q if (i // q) % 2 == 0 else i - q) for i in range(groups)
    ]
    cores = [(i, i ^ 1) for i in range(groups)]
    crossed = lax.ppermute(own, "modes", middle)
    w1 = turned(branch_one, leg_orders[0], "turn_one")
    cut, crossed, w1, branch_two = lax.optimization_barrier((cut, crossed, w1, branch_two))
    arrived = lax.all_to_all(cut, "modes", split_axis=0, concat_axis=0, tiled=True)
    x = arrived.reshape(groups * entries, 8 * lanes)
    w2 = turned(branch_two, leg_orders[1], "turn_two")
    crossed, w2 = lax.optimization_barrier((crossed, w2))
    inner = (quarter == 1) | (quarter == 2)
    wa = jnp.where(inner, crossed, own)
    wb = lax.ppermute(wa, "modes", outer)
    wc = lax.ppermute(wa, "modes", cores)
    wd = lax.ppermute(wb, "modes", cores)

    width = w1.shape[1]
    half = width // 2
    any_spec = pl.BlockSpec(memory_space=pl.ANY)
    vmem = pl.BlockSpec(memory_space=pltpu.VMEM)
    values = pl.pallas_call(
        two_branches,
        name="two_branches",
        out_shape=jax.ShapeDtypeStruct((4, half, 4 * lanes), jnp.bfloat16),
        in_specs=[any_spec] * 3,
        out_specs=vmem,
        scratch_shapes=[
            pltpu.VMEM(x.shape, x.dtype),
            pltpu.VMEM(w1.shape, w1.dtype),
            pltpu.VMEM(w2.shape, w2.dtype),
            pltpu.VMEM((width, 8 * lanes), jnp.bfloat16),
            pltpu.SemaphoreType.DMA((1 + 2 * TILES,)),
        ],
        compiler_params=pltpu.CompilerParams(vmem_limit_bytes=58 * 2**20),
        cost_estimate=pl.CostEstimate(
            flops=8 * width * width * 8 * lanes, bytes_accessed=12 * 2**20, transcendentals=0
        ),
    )(x, w1, w2)

    out_width = own.shape[1]
    partial = pl.pallas_call(
        third_branch,
        name="third_branch",
        out_shape=jax.ShapeDtypeStruct((out_width, 4 * lanes), jnp.bfloat16),
        in_specs=[pl.BlockSpec(memory_space=pltpu.SMEM)] + [vmem] * 5,
        out_specs=vmem,
        compiler_params=pltpu.CompilerParams(vmem_limit_bytes=24 * 2**20),
        cost_estimate=pl.CostEstimate(
            flops=16 * out_width * half * 4 * lanes, bytes_accessed=7 * 2**20, transcendentals=0
        ),
    )(jnp.stack([k2, k0]).astype(jnp.int32), wa, wb, wc, wd, values)

    pieces = lax.all_to_all(partial, "modes", split_axis=0, concat_axis=0, tiled=True)
    mine = out_width // groups
    pieces = pieces.reshape(2, 2, rest, 2, mine, 2, 2, lanes).astype(jnp.float32)
    summed = jnp.sum(pieces, axis=(0, 2)).astype(jnp.bfloat16)
    return summed.transpose(2, 3, 4, 1, 0, 5).reshape(mine, 2, 2, 2, 2 * lanes)


def solution(mesh):
    in_specs = (
        P(None, "modes", None, None, "parts"),
        P(),
        P(),
        P(None, None, "modes", None, None),
        P(),
        P("parts"),
    )
    out_specs = P(("parts", "modes"), None, None, None, None)
    return jax.shard_map(
        per_device, mesh=mesh, in_specs=in_specs, out_specs=out_specs, check_vma=False
    )
```

```python
import jax
import jax.numpy as jnp
from jax import lax
from jax.experimental import pallas as pl
from jax.experimental.pallas import tpu as pltpu
from jax.sharding import PartitionSpec as P

TILES = 4


def turn_columns(order, branch, out, onehot):
    width = branch.shape[1]

    @pl.when(pl.program_id(0) == 0)
    def _():
        positions = lax.broadcasted_iota(jnp.int32, (1, width), 1)
        source = jnp.zeros((1, width), jnp.int32)
        for bit in range(order.shape[0]):
            source += jnp.left_shift(jnp.right_shift(positions, bit) & 1, order[bit])
        rows = lax.broadcasted_iota(jnp.int32, (width, width), 0)
        onehot[...] = jnp.where(rows == source, 1.0, 0.0).astype(onehot.dtype)

    out[...] = jnp.dot(
        branch[...], onehot[...], preferred_element_type=jnp.float32
    ).astype(out.dtype)


def turned(branch, order, name):
    width = branch.shape[2]
    flat = branch.reshape(-1, width)
    tile = flat.shape[0] // 8
    out = pl.pallas_call(
        turn_columns,
        name=name,
        grid=(8,),
        out_shape=jax.ShapeDtypeStruct(flat.shape, flat.dtype),
        in_specs=[
            pl.BlockSpec(memory_space=pltpu.SMEM),
            pl.BlockSpec((tile, width), lambda i: (i, 0)),
        ],
        out_specs=pl.BlockSpec((tile, width), lambda i: (i, 0)),
        scratch_shapes=[pltpu.VMEM((width, width), flat.dtype)],
        compiler_params=pltpu.CompilerParams(vmem_limit_bytes=58 * 2**20),
        cost_estimate=pl.CostEstimate(
            flops=2 * flat.shape[0] * width * width,
            bytes_accessed=4 * flat.size,
            transcendentals=0,
        ),
    )(order, flat)
    return out.reshape(branch.shape)


def complex_tile(w, values):
    half = values.shape[1] // 2
    p = jnp.dot(w[0], values, preferred_element_type=jnp.float32)
    q = jnp.dot(w[1], values, preferred_element_type=jnp.float32)
    real = p[:, :half] - q[:, half:]
    imag = p[:, half:] + q[:, :half]
    return real.astype(jnp.bfloat16), imag.astype(jnp.bfloat16)


def two_branches(x_hbm, w1_hbm, w2_hbm, out, x, w1, w2, mid, sems):
    width = x.shape[0]
    half = width // 2
    tile = width // TILES
    lanes = x.shape[1] // 8
    copies = [pltpu.make_async_copy(x_hbm, x, sems.at[0])]
    for which, (source, target) in enumerate(((w1_hbm, w1), (w2_hbm, w2))):
        for i in range(TILES):
            rows = pl.ds(i * tile, tile)
            copies.append(
                pltpu.make_async_copy(
                    source.at[:, rows, :], target.at[:, rows, :], sems.at[1 + which * TILES + i]
                )
            )
    for copy in copies:
        copy.start()
    copies[0].wait()
    for i in range(TILES):
        copies[1 + i].wait()
        t, c = divmod(i * tile, half)
        parts = complex_tile(w1[:, i * tile : (i + 1) * tile, :], x[...])
        for r in range(2):
            for a in range(2):
                at = (2 * r + t) * 2 * lanes
                mid[a * half + c : a * half + c + tile, at : at + 2 * lanes] = parts[r][
                    :, a * 2 * lanes : (a + 1) * 2 * lanes
                ]
    for i in range(TILES):
        copies[1 + TILES + i].wait()
        u, c = divmod(i * tile, half)
        parts = complex_tile(w2[:, i * tile : (i + 1) * tile, :], mid[...])
        for r in range(2):
            for td in range(4):
                at = (2 * r + u) * lanes
                out[td, c : c + tile, at : at + lanes] = parts[r][:, td * lanes : (td + 1) * lanes]


def third_branch(place, ar, ai, br, bi, cr, ci, dr, di, values, out):
    k2 = place[0]
    k0 = place[1]
    half = values.shape[2] // 2
    p = q = None
    sources = (
        (ar, ai, k2, k0),
        (br, bi, 1 - k2, k0),
        (cr, ci, k2, 1 - k0),
        (dr, di, 1 - k2, 1 - k0),
    )
    for real, imag, t, d in sources:
        block = values[2 * t + d]
        pp = jnp.dot(real[...], block, preferred_element_type=jnp.float32)
        qq = jnp.dot(imag[...], block, preferred_element_type=jnp.float32)
        p = pp if p is None else p + pp
        q = qq if q is None else q + qq
    out[:, :half] = (p[:, :half] - q[:, half:]).astype(out.dtype)
    out[:, half:] = (p[:, half:] + q[:, :half]).astype(out.dtype)


def per_device(stem, branch_one, branch_two, branch_three, leg_orders, slice_pick):
    groups = lax.axis_size("modes")
    me = lax.axis_index("modes")
    rest = groups // 8
    entries, lanes = stem.shape[2], stem.shape[4] // 2
    k2 = (me // (2 * rest)) % 2
    quarter = me // (2 * rest)
    k0 = me % 2

    cut = stem.reshape(2, entries, 2, 2, rest, 2, 2, 2, lanes)
    cut = cut.transpose(3, 7, 4, 5, 1, 0, 2, 6, 8).reshape(groups, entries, 8 * lanes)
    pick = lax.dynamic_index_in_dim(slice_pick, me, 0, keepdims=False)
    own = lax.dynamic_index_in_dim(branch_three, pick, 0, keepdims=False)[:, 0]
    q = 2 * rest
    middle = [(q + i, 2 * q + i) for i in range(q)]
    middle += [(b, a) for a, b in middle]
    outer = [(i, i ^ q) for i in range(groups)] if q & (q - 1) == 0 else [
        (i, i + q if (i // q) % 2 == 0 else i - q) for i in range(groups)
    ]
    cores = [(i, i ^ 1) for i in range(groups)]
    inner = (quarter == 1) | (quarter == 2)
    crossed_real = lax.ppermute(own[0], "modes", middle)
    wa_real = jnp.where(inner, crossed_real, own[0])
    wb_real = lax.ppermute(wa_real, "modes", outer)
    crossed = lax.ppermute(own[1], "modes", middle)
    w1 = turned(branch_one, leg_orders[0], "turn_one")
    cut, crossed, w1, branch_two = lax.optimization_barrier((cut, crossed, w1, branch_two))
    arrived = lax.all_to_all(cut, "modes", split_axis=0, concat_axis=0, tiled=True)
    x = arrived.reshape(groups * entries, 8 * lanes)
    w2 = turned(branch_two, leg_orders[1], "turn_two")
    crossed, w2 = lax.optimization_barrier((crossed, w2))
    wa_imag = jnp.where(inner, crossed, own[1])
    wb_imag = lax.ppermute(wa_imag, "modes", outer)
    wc_real = lax.ppermute(wa_real, "modes", cores)
    wc_imag = lax.ppermute(wa_imag, "modes", cores)
    wd_real = lax.ppermute(wb_real, "modes", cores)
    wd_imag = lax.ppermute(wb_imag, "modes", cores)
    blocks = (wa_real, wa_imag, wb_real, wb_imag, wc_real, wc_imag, wd_real, wd_imag)

    width = w1.shape[1]
    half = width // 2
    any_spec = pl.BlockSpec(memory_space=pl.ANY)
    vmem = pl.BlockSpec(memory_space=pltpu.VMEM)
    values = pl.pallas_call(
        two_branches,
        name="two_branches",
        out_shape=jax.ShapeDtypeStruct((4, half, 4 * lanes), jnp.bfloat16),
        in_specs=[any_spec] * 3,
        out_specs=vmem,
        scratch_shapes=[
            pltpu.VMEM(x.shape, x.dtype),
            pltpu.VMEM(w1.shape, w1.dtype),
            pltpu.VMEM(w2.shape, w2.dtype),
            pltpu.VMEM((width, 8 * lanes), jnp.bfloat16),
            pltpu.SemaphoreType.DMA((1 + 2 * TILES,)),
        ],
        compiler_params=pltpu.CompilerParams(vmem_limit_bytes=58 * 2**20),
        cost_estimate=pl.CostEstimate(
            flops=8 * width * width * 8 * lanes, bytes_accessed=12 * 2**20, transcendentals=0
        ),
    )(x, w1, w2)

    out_width = own.shape[1]
    partial = pl.pallas_call(
        third_branch,
        name="third_branch",
        out_shape=jax.ShapeDtypeStruct((out_width, 4 * lanes), jnp.bfloat16),
        in_specs=[pl.BlockSpec(memory_space=pltpu.SMEM)] + [vmem] * 9,
        out_specs=vmem,
        compiler_params=pltpu.CompilerParams(vmem_limit_bytes=24 * 2**20),
        cost_estimate=pl.CostEstimate(
            flops=16 * out_width * half * 4 * lanes, bytes_accessed=7 * 2**20, transcendentals=0
        ),
    )(jnp.stack([k2, k0]).astype(jnp.int32), *blocks, values)

    pieces = lax.all_to_all(partial, "modes", split_axis=0, concat_axis=0, tiled=True)
    mine = out_width // groups
    pieces = pieces.reshape(2, 2, rest, 2, mine, 2, 2, lanes).astype(jnp.float32)
    summed = jnp.sum(pieces, axis=(0, 2)).astype(jnp.bfloat16)
    return summed.transpose(2, 3, 4, 1, 0, 5).reshape(mine, 2, 2, 2, 2 * lanes)


def solution(mesh):
    in_specs = (
        P(None, "modes", None, None, "parts"),
        P(),
        P(),
        P(None, None, "modes", None, None),
        P(),
        P("parts"),
    )
    out_specs = P(("parts", "modes"), None, None, None, None)
    return jax.shard_map(
        per_device, mesh=mesh, in_specs=in_specs, out_specs=out_specs, check_vma=False
    )
```
